512 devices in a mesh: ep: 64 (over x, z), rep: 8 (over y, core).
Axes of the slice: x: 4, y: 4, z: 16, core: 2. Of those that a mesh axis runs over, the one named last changes fastest.
Arguments:
- tokens: bfloat16 [65536, 1024], P(('ep', 'rep')), may hold values from -6 to 6
- expert_ids: int32 [65536, 6], P(('ep', 'rep')), may hold values from 0 to 63, all different within a row; in each aligned block of 128 rows (0 to 127, 128 to 255, ...) at most 13 rows name the same one
- gate_weights: float32 [65536, 6], P(('ep', 'rep')), may hold values from 0.1 to 0.5
- cotangent: bfloat16 [65536, 1024], P(('ep', 'rep')), may hold values from -6 to 6
- w_gate: bfloat16 [64, 1024, 704], P('ep', 'rep'), may hold values from -0.1875 to 0.1875
- w_up: bfloat16 [64, 1024, 704], P('ep', 'rep'), may hold values from -0.1875 to 0.1875
- w_down: bfloat16 [64, 704, 1024], P('ep', None, 'rep'), may hold values from -0.21875 to 0.21875
Outputs:
- mixed_out: bfloat16 [65536, 1024], P(('ep', 'rep'))
- grad_up: float32 [64, 1024, 704], P('ep', 'rep')
- grad_down: float32 [64, 704, 1024], P('ep', None, 'rep')
The draws below stay inside these ranges and needn't reach their ends.
Inputs may be any that keep to these rules, and one draw needn't show every extreme that they name: `expert_ids`: each token names 6 different experts. Of the tokens of one device, at most 13 name any one expert, and in every draw some expert is named by exactly 13 of some device's tokens.
All inputs are finite; a program needn't handle non-finite values.
Results may differ from the reference program's by a relative error of at most 0.012.
Values may be sent and summed in bfloat16 or wider, within the bound.
No kernel may reach another device: no remote copies, remote signals or barrier semaphores. Data moves between devices by JAX's collectives and lax.ppermute only.
A program may use at most 128 MiB of HBM per device.

```python
import math
import jax
import jax.numpy as jnp
import numpy as np
from jax import lax

D = 1024
H = 704
TOP = 6
TOK_DEV = 128
EXPERTS = 64
CAP = 13
TOKENS = 65536
N_EP = 64
N_REP = 8


def block_scale(own_key, shape, split, low, high):
    factor_of, own = 1.0, jax.random.fold_in(own_key, 6)
    for dim, shards_of in split:
        heights = jnp.exp(jax.random.uniform(jax.random.fold_in(own, dim), (shards_of,), jnp.float32, low / len(split), high / len(split)))
        factor_of = factor_of * jnp.repeat(heights, shape[dim] // shards_of).reshape([-1 if axis == dim else 1 for axis in range(len(shape))])
    return factor_of


def routed_block(rng, own, number, rows, count, top, bound, slope):
    sequence = jax.random.permutation(rng, count)
    heavy_load, usual = portions_of(count, rows * top, bound, slope, True), portions_of(count, rows * top, bound, slope, False)
    places = jnp.arange(count)

    def named(sizes, rotation):
        used = int((sizes > 0).sum())
        fixed = max(1, used // 4)
        passed = fixed + (places - fixed + rotation * (used - fixed)) % max(1, count - fixed)
        return jnp.zeros((count,), jnp.int32).at[sequence[jnp.where(places < fixed, places, passed)]].set(jnp.asarray(sizes, jnp.int32))

    sizes = jnp.where(number % 4 == 0, named(heavy_load, number // 4), named(usual, number - number // 4 - 1))
    mixed = jax.random.permutation(jax.random.fold_in(own, 3), count)
    donor, sink = mixed[0:count // 2 * 2:2], mixed[1:count // 2 * 2:2]
    room = jnp.minimum(sizes[donor] - 1, bound - sizes[sink]) // 2
    room = jnp.where((donor == sequence[0]) | (sink == sequence[0]) | (sizes[sink] == 0), 0, jnp.maximum(room, 0))
    passed = jax.random.randint(jax.random.fold_in(own, 4), (count // 2,), 0, 1 << 20) % (room + 1)
    sizes = sizes.at[donor].add(-passed).at[sink].add(passed)
    members = jnp.searchsorted(jnp.cumsum(sizes), jnp.arange(rows * top), side="right").astype(jnp.int32)
    table = members.reshape(top, rows).T
    table = table[jax.random.permutation(jax.random.fold_in(own, 1), rows)]
    rotation = jax.random.randint(jax.random.fold_in(own, 2), (rows, 1), 0, top)
    return jnp.take_along_axis(table, (jnp.arange(top)[None, :] + rotation) % top, axis=1)


def portions_of(count, total, most, lean, full):
    loads = [(1 << 20) // math.isqrt(rank ** lean) + 1 for rank in range(1, count + 1)]
    largest = most if full else min(most, max(-(-total // count), total * loads[0] // sum(loads)))
    least = 1 if total - largest >= count - 1 else 0
    holding, spare = [largest] + [least] * (count - 1), total - largest - least * (count - 1)
    while spare > 0:
        movable = [i for i in range(1, count) if holding[i] < largest] or [i for i in range(1, count) if holding[i] < most]
        whole, left = sum([loads[i] for i in movable]), spare
        for i in movable:
            extra = min(most - holding[i], max(1, left * loads[i] // whole), spare)
            holding[i] = holding[i] + extra
            spare = spare - extra
    return np.array(holding)


def bell_draw(rng, dims, spread, most, split=(), kind=jnp.bfloat16):
    level = block_scale(rng, dims, split, -0.22, 0.18) if split else 1.0
    drawn = jax.random.normal(rng, dims, jnp.float32) * spread * level
    return jnp.minimum(jnp.maximum(drawn, -most), most).astype(kind)


def setup_inputs(seed: int = 0) -> dict:
    key_list = jax.random.split(jax.random.key(seed), 8)
    tokens = bell_draw(key_list[0], (TOKENS, D), 1.0, 6.0, ((0, 512),))
    expert_ids_keys = jax.random.split(jax.random.fold_in(key_list[1], 1), TOKENS // TOK_DEV)
    expert_ids_turns = jax.random.permutation(jax.random.fold_in(key_list[1], 3), TOKENS // TOK_DEV)
    expert_ids = jax.vmap(lambda own, number: routed_block(jax.random.fold_in(key_list[1], 2), own, number, TOK_DEV, EXPERTS, TOP, CAP, 2))(expert_ids_keys, expert_ids_turns).reshape((TOKENS, TOP))
    gate_weights = jnp.clip(0.1 + 0.4 * jax.random.uniform(key_list[2], (TOKENS, TOP), jnp.float32) ** block_scale(key_list[2], (TOKENS, TOP), ((0, 512),), -0.2, 0.2), 0.1, 0.5)
    cotangent = bell_draw(key_list[3], (TOKENS, D), 1.0, 6.0, ((0, 512),))
    w_gate = bell_draw(key_list[4], (EXPERTS, D, H), D ** -0.5, 0.1875, ((0, 64), (1, 8)))
    w_up = bell_draw(key_list[5], (EXPERTS, D, H), D ** -0.5, 0.1875, ((0, 64), (1, 8)))
    w_down = bell_draw(key_list[6], (EXPERTS, H, D), H ** -0.5, 0.21875, ((0, 64), (2, 8)))
    return {"tokens": tokens, "expert_ids": expert_ids, "gate_weights": gate_weights, "cotangent": cotangent, "w_gate": w_gate, "w_up": w_up, "w_down": w_down}


def reference(tokens, expert_ids, gate_weights, cotangent, w_gate, w_up, w_down):
    devices = N_EP * N_REP
    pair_count = TOK_DEV * TOP
    flat_ids = expert_ids.reshape(devices, pair_count).astype(jnp.int32)
    one_hot = (flat_ids[:, :, None] == jnp.arange(EXPERTS, dtype=jnp.int32)[None, None, :]).astype(jnp.int32)
    position = jnp.sum(one_hot * jnp.cumsum(one_hot, axis=1), axis=2) - 1
    device = jnp.arange(devices, dtype=jnp.int32)[:, None]
    source = device // N_REP
    rep_group = device % N_REP
    slot_index = (((flat_ids * N_REP + rep_group) * N_EP + source) * CAP + position).reshape(-1)
    slot_total = EXPERTS * N_REP * N_EP * CAP
    pair_index = jnp.arange(devices * pair_count, dtype=jnp.int32)
    owner_pair = jnp.zeros((slot_total,), jnp.int32).at[slot_index].set(pair_index)
    filled = jnp.zeros((slot_total,), jnp.float32).at[slot_index].set(1.0)
    owner_pair = owner_pair.reshape(EXPERTS, N_REP * N_EP * CAP)
    filled = filled.reshape(EXPERTS, N_REP * N_EP * CAP)
    gate_flat = gate_weights.reshape(-1).astype(jnp.float32)

    def expert_step(running, inputs):
        expert_owner, expert_filled, gate_shard, up_shard, down_shard = inputs
        token_rows = expert_owner // TOP
        arrived = tokens[token_rows] * expert_filled[:, None].astype(jnp.bfloat16)
        pair_scale = gate_flat[expert_owner] * expert_filled
        grad_rows = (pair_scale[:, None] * cotangent[token_rows].astype(jnp.float32)).astype(jnp.bfloat16)
        gate_pre = jnp.dot(arrived, gate_shard, preferred_element_type=jnp.float32)
        up_pre = jnp.dot(arrived, up_shard, preferred_element_type=jnp.float32)
        hidden = (jax.nn.silu(gate_pre) * up_pre).astype(jnp.bfloat16)
        expert_out = jnp.dot(hidden, down_shard, preferred_element_type=jnp.float32).astype(jnp.bfloat16)
        running = running.at[token_rows].add(pair_scale[:, None] * expert_out.astype(jnp.float32))
        hidden_grad = lax.dot_general(grad_rows, down_shard, (((1,), (1,)), ((), ())), preferred_element_type=jnp.float32)
        up_grad = (hidden_grad * jax.nn.silu(gate_pre)).astype(jnp.bfloat16)
        rows_group = arrived.reshape(N_REP, N_EP * CAP, D).astype(jnp.float32)
        up_group = up_grad.reshape(N_REP, N_EP * CAP, H).astype(jnp.float32)
        hidden_group = hidden.reshape(N_REP, N_EP * CAP, H).astype(jnp.float32)
        grad_group = grad_rows.reshape(N_REP, N_EP * CAP, D).astype(jnp.float32)
        part_up = jnp.einsum("grd,grh->gdh", rows_group, up_group, precision=lax.Precision.HIGHEST)
        part_down = jnp.einsum("grh,grd->ghd", hidden_group, grad_group, precision=lax.Precision.HIGHEST)
        part_up = lax.optimization_barrier(part_up.astype(jnp.bfloat16)).astype(jnp.float32)
        part_down = lax.optimization_barrier(part_down.astype(jnp.bfloat16)).astype(jnp.float32)
        return running, (jnp.sum(part_up, axis=0), jnp.sum(part_down, axis=0))

    start_sum = jnp.zeros((TOKENS, D), jnp.float32)
    mixed_sum, grads = lax.scan(expert_step, start_sum, (owner_pair, filled, w_gate, w_up, w_down))
    return mixed_sum.astype(jnp.bfloat16), grads[0], grads[1]
```

```python
import functools

import jax
import jax.numpy as jnp
from jax import lax
from jax.experimental import pallas as pl
from jax.experimental.pallas import tpu as pltpu
from jax.sharding import PartitionSpec as P

NX, NZ = 4, 16
CAP = 13
TOP = 6
TOK = 128
EXTRA = 8
NEAR = (0, 1, 2, 3, 4, -1, -2, -3)
FAR = (5, 6, 7, -4, -5, -6, -7, 8)
COUNT = len(NEAR)
ROWS = CAP * COUNT
PAD = 128
ZG = [[x * NZ + z for z in range(NZ)] for x in range(NX)]
XG = [[x * NZ + z for x in range(NX)] for z in range(NZ)]


def zperm(d):
    return [(x * NZ + z, x * NZ + (z + d) % NZ) for x in range(NX) for z in range(NZ)]


def pack_body(tokens_ref, ids_ref, gates_ref, out_ref):
    out_ref[:TOK, :] = tokens_ref[...]
    gates = gates_ref[...]
    high = gates.astype(jnp.bfloat16).astype(jnp.float32)
    mid = (gates - high).astype(jnp.bfloat16).astype(jnp.float32)
    low = gates - high - mid
    ids = ids_ref[...].astype(jnp.float32)
    blank = jnp.zeros((EXTRA - 4, TOK), jnp.float32)
    for k in range(TOP):
        at = slice(k, k + 1)
        rows = jnp.concatenate([ids[at], high[at], mid[at], low[at], blank], axis=0)
        out_ref[TOK:, k * TOK : (k + 1) * TOK] = rows.astype(jnp.bfloat16)
    rest = out_ref.shape[1] - TOP * TOK
    out_ref[TOK:, TOP * TOK :] = jnp.zeros((EXTRA, rest), jnp.bfloat16)


def pack(tokens, ids, gates):
    return pl.pallas_call(
        pack_body,
        out_shape=jax.ShapeDtypeStruct((TOK + EXTRA, tokens.shape[1]), jnp.bfloat16),
        cost_estimate=pl.CostEstimate(flops=0, bytes_accessed=4 * TOK * tokens.shape[1], transcendentals=0),
        name="pack",
    )(tokens, ids.T, gates.T)


def ring(a):
    held = {0: (a,)}
    fwd = back = a
    half = NZ // 2
    for i in range(1, half):
        fwd = lax.ppermute(fwd, "ep", zperm(1))
        back = lax.ppermute(back, "ep", zperm(-1))
        held[i], held[-i] = (fwd,), (back,)
    mid = TOK // 2
    held[half] = (
        lax.ppermute(fwd[:mid], "ep", zperm(1)),
        lax.ppermute(back[mid:], "ep", zperm(-1)),
    )
    return held


def pick_rows(code, gate, all_rows, out_ref, weighted):
    slot = lax.broadcasted_iota(jnp.int32, (ROWS, all_rows.shape[0]), 0)
    for j in range(NX):
        hit = slot == code[j : j + 1, :]
        got = jnp.dot(
            jnp.where(hit, 1.0, 0.0).astype(jnp.bfloat16), all_rows, preferred_element_type=jnp.float32
        )
        if weighted:
            got = got * jnp.sum(jnp.where(hit, gate[j : j + 1, :], 0.0), axis=1, keepdims=True)
        out_ref[j] = got.astype(jnp.bfloat16)


def pick_body(place_ref, *refs, spots):
    chunks, (out_ref, code_ref, gate_ref, code_t_ref, gate_t_ref, stage, extra) = refs[:-7], refs[-7:]
    for c, (n, row) in zip(chunks, spots):
        end = row + c.shape[0]
        if end <= TOK:
            stage[n * TOK + row : n * TOK + end, :] = c[...]
        else:
            stage[n * TOK + row : (n + 1) * TOK, :] = c[: TOK - row, :]
            extra[n * EXTRA : (n + 1) * EXTRA, :] = c[TOK - row :, :].astype(jnp.float32)
    mine = place_ref[0] + NZ * lax.broadcasted_iota(jnp.int32, (NX, TOK), 0)
    mine = mine.astype(jnp.float32)
    hits, weights = [], []
    for n in range(COUNT):
        hit = jnp.zeros((NX, TOK), jnp.float32)
        weight = jnp.zeros((NX, TOK), jnp.float32)
        for k in range(TOP):
            part = extra[n * EXTRA : n * EXTRA + 4, k * TOK : (k + 1) * TOK]
            same = part[0:1] == mine
            hit = jnp.where(same, 1.0, hit)
            weight = jnp.where(same, part[1:2] + part[2:3] + part[3:4], weight)
        hits.append(hit)
        weights.append(weight)
    hits, weights = jnp.concatenate(hits, axis=0), jnp.concatenate(weights, axis=0)
    shape = (TOK, TOK)
    earlier = lax.broadcasted_iota(jnp.int32, shape, 0) < lax.broadcasted_iota(jnp.int32, shape, 1)
    position = jnp.dot(
        hits.astype(jnp.bfloat16),
        jnp.where(earlier, 1.0, 0.0).astype(jnp.bfloat16),
        preferred_element_type=jnp.float32,
    )
    first = CAP * (lax.broadcasted_iota(jnp.int32, (NX * COUNT, TOK), 0) // NX)
    codes = jnp.where(hits > 0, position.astype(jnp.int32) + first, -1)
    codes_f = codes.astype(jnp.float32)
    fill = jnp.zeros((TOK - NX * COUNT, TOK), jnp.float32)
    code_t = jnp.concatenate([codes_f, fill], axis=0).T
    gate_t = jnp.concatenate([weights, fill], axis=0).T
    for n in range(COUNT):
        at = slice(n * NX, (n + 1) * NX)
        code_ref[:, n * TOK : (n + 1) * TOK] = codes[at]
        gate_ref[:, n * TOK : (n + 1) * TOK] = weights[at]
        code_t_ref[n] = code_t[:, at]
        gate_t_ref[n] = gate_t[:, at]
    pick_rows(code_ref[...], None, stage[...], out_ref, False)


def pick_cost(rows, width):
    return pl.CostEstimate(
        flops=2 * NX * ROWS * rows * width, bytes_accessed=2 * (rows + NX * ROWS) * width, transcendentals=0
    )


def pick(place, groups):
    pieces, spots = [], []
    for n, group in enumerate(groups):
        row = 0
        for piece in group:
            pieces.append(piece)
            spots.append((n, row))
            row += piece.shape[0]
    width = pieces[0].shape[1]
    rows = COUNT * TOK
    shapes = [((NX, ROWS, width), jnp.bfloat16), ((NX, rows), jnp.int32), ((NX, rows), jnp.float32)]
    shapes += [((COUNT, TOK, NX), jnp.float32)] * 2
    return pl.pallas_call(
        functools.partial(pick_body, spots=spots),
        out_shape=[jax.ShapeDtypeStruct(s, t) for s, t in shapes],
        in_specs=[pl.BlockSpec(memory_space=pltpu.SMEM)] + [pl.BlockSpec(memory_space=pltpu.VMEM)] * len(pieces),
        scratch_shapes=[pltpu.VMEM((rows, width), jnp.bfloat16), pltpu.VMEM((COUNT * EXTRA, width), jnp.float32)],
        cost_estimate=pick_cost(rows, width),
        name="pick",
    )(place, *pieces)


def pick_from_body(source_ref, code_ref, gate_ref, *refs):
    chunks, out_ref, stage = refs[:-2], refs[-2], refs[-1]
    for n, c in enumerate(chunks):
        stage[n * TOK : (n + 1) * TOK, :] = c[...]
    pick_rows(code_ref[...], gate_ref[...], stage[...], out_ref, True)


def pick_from(source, code, gate, gathered):
    width = gathered.shape[1]
    rows = COUNT * TOK
    small = pl.BlockSpec((NX, rows), lambda i, source: (0, 0))
    chunk = [pl.BlockSpec((TOK, width), lambda i, source, n=n: (source[n], 0)) for n in range(COUNT)]
    return pl.pallas_call(
        pick_from_body,
        out_shape=jax.ShapeDtypeStruct((NX, ROWS, width), jnp.bfloat16),
        grid_spec=pltpu.PrefetchScalarGridSpec(
            num_scalar_prefetch=1,
            grid=(1,),
            in_specs=[small, small] + chunk,
            out_specs=pl.BlockSpec((NX, ROWS, width), lambda i, source: (0, 0, 0)),
            scratch_shapes=[pltpu.VMEM((rows, width), jnp.bfloat16)],
        ),
        cost_estimate=pick_cost(rows, width),
        name="pick_weighted",
    )(source, code, gate, *([gathered] * COUNT))


def mix_body(dest_ref, code_ref, gate_ref, rows_ref, *refs):
    out_ref, stage = refs[-2], refs[-1]
    width = out_ref.shape[1]

    @pl.when(pl.program_id(0) == 0)
    def _():
        for j in range(NX):
            stage[j * PAD : j * PAD + ROWS, :] = rows_ref[j]
            stage[j * PAD + ROWS : (j + 1) * PAD, :] = jnp.zeros((PAD - ROWS, width), jnp.bfloat16)

    slot = lax.broadcasted_iota(jnp.int32, (TOK, PAD), 1).astype(jnp.float32)
    code, gate = code_ref[0], gate_ref[0]
    full = jnp.concatenate(
        [jnp.where(slot == code[:, j : j + 1], gate[:, j : j + 1], 0.0) for j in range(NX)], axis=1
    )
    high = full.astype(jnp.bfloat16)
    low = (full - high.astype(jnp.float32)).astype(jnp.bfloat16)
    both = jnp.dot(jnp.concatenate([high, low], axis=0), stage[...], preferred_element_type=jnp.float32)
    out_ref[...] = (both[:TOK] + both[TOK:]).astype(jnp.bfloat16)


def mix(dest, code_t, gate_t, rows, before):
    width = rows.shape[2]
    small = pl.BlockSpec((1, TOK, NX), lambda i, dest: (i, 0, 0))
    chained = before is not None
    return pl.pallas_call(
        mix_body,
        out_shape=jax.ShapeDtypeStruct((NZ * TOK, width), jnp.bfloat16),
        grid_spec=pltpu.PrefetchScalarGridSpec(
            num_scalar_prefetch=1,
            grid=(COUNT,),
            in_specs=[small, small, pl.BlockSpec((NX, ROWS, width), lambda i, dest: (0, 0, 0))]
            + ([pl.BlockSpec(memory_space=pl.ANY)] if chained else []),
            out_specs=pl.BlockSpec((TOK, width), lambda i, dest: (dest[i], 0)),
            scratch_shapes=[pltpu.VMEM((NX * PAD, width), jnp.bfloat16)],
        ),
        input_output_aliases={4: 0} if chained else {},
        cost_estimate=pl.CostEstimate(
            flops=4 * NX * PAD * COUNT * TOK * width,
            bytes_accessed=2 * (NX * ROWS + COUNT * TOK) * width,
            transcendentals=0,
        ),
        name="mix",
    )(dest, code_t, gate_t, rows, *((before,) if chained else ()))


def across_x(blocks):
    return lax.all_to_all(blocks, "ep", split_axis=0, concat_axis=0, axis_index_groups=XG, tiled=True)


def local(tokens, expert_ids, gate_weights, cotangent, w_gate, w_up, w_down):
    width = tokens.shape[1]
    z = lax.axis_index("ep") % NZ
    n_rep = lax.axis_size("rep")
    all_cot = lax.all_gather(cotangent, "ep", axis_index_groups=ZG, axis=0, tiled=True)
    held = ring(pack(tokens, expert_ids, gate_weights))
    source = (z - jnp.array(NEAR + FAR, jnp.int32)) % NZ
    place = z.reshape(1)

    hidden_width = w_gate.shape[2]
    share = w_gate.shape[1]
    shards = jnp.concatenate([w_gate[0].T, w_up[0].T, w_down[0]], axis=1)
    shards, _, _ = lax.optimization_barrier((shards, held[1][0], held[-1][0]))
    shards = jnp.broadcast_to(shards[None], (n_rep,) + shards.shape)
    shards = lax.all_to_all(shards, "rep", split_axis=0, concat_axis=0, tiled=True)
    full_gate, full_up, full_down = (
        shards[:, :, n * share : (n + 1) * share].transpose(1, 0, 2).reshape(hidden_width, width)
        for n in range(3)
    )
    last = (((1,), (1,)), ((), ()))
    first = (((0,), (0,)), ((), ()))

    mixed = None
    kept = []
    for b, group in enumerate((NEAR, FAR)):
        sources = source[b * COUNT : (b + 1) * COUNT]
        rows, code, gate, code_t, gate_t = pick(place, [held[d] for d in group])
        rows = across_x(rows).reshape(NX * ROWS, width)
        gate_pre = lax.dot_general(rows, full_gate, last, preferred_element_type=jnp.float32)
        up_pre = lax.dot_general(rows, full_up, last, preferred_element_type=jnp.float32)
        silu = jax.nn.silu(gate_pre)
        hidden = (silu * up_pre).astype(jnp.bfloat16)
        out = jnp.dot(hidden, full_down, preferred_element_type=jnp.float32).astype(jnp.bfloat16)
        mixed = mix(sources, code_t, gate_t, across_x(out.reshape(NX, ROWS, width)), mixed)
        kept.append((sources, code, gate, rows, silu, hidden))
    mixed_out = lax.psum_scatter(mixed, "ep", axis_index_groups=ZG, scatter_dimension=0, tiled=True)

    part_up = part_down = None
    for sources, code, gate, rows, silu, hidden in kept:
        grad_rows = across_x(pick_from(sources, code, gate, all_cot)).reshape(NX * ROWS, width)
        hidden_grad = lax.dot_general(grad_rows, full_down, last, preferred_element_type=jnp.float32)
        up_grad = (hidden_grad * silu).astype(jnp.bfloat16)
        down = lax.dot_general(grad_rows, hidden, first, preferred_element_type=jnp.float32)
        up = lax.dot_general(rows, up_grad, first, preferred_element_type=jnp.float32)
        part_down = down if part_down is None else part_down + down
        part_up = up if part_up is None else part_up + up

    def summed(part):
        part = part.astype(jnp.bfloat16).reshape(n_rep, width // n_rep, hidden_width)
        part = lax.all_to_all(part, "rep", split_axis=0, concat_axis=0, tiled=True)
        return jnp.sum(part.astype(jnp.float32), axis=0)

    grad_down = summed(part_down).T
    grad_up = summed(part_up)
    return mixed_out, grad_up[None], grad_down[None]


def solution(mesh):
    in_specs = (
        P(("ep", "rep"), None),
        P(("ep", "rep"), None),
        P(("ep", "rep"), None),
        P(("ep", "rep"), None),
        P("ep", "rep", None),
        P("ep", "rep", None),
        P("ep", None, "rep"),
    )
    out_specs = (P(("ep", "rep"), None), P("ep", "rep", None), P("ep", None, "rep"))
    return jax.shard_map(local, mesh=mesh, in_specs=in_specs, out_specs=out_specs, check_vma=False)
```

```python
import functools

import jax
import jax.numpy as jnp
from jax import lax
from jax.experimental import pallas as pl
from jax.experimental.pallas import tpu as pltpu
from jax.sharding import PartitionSpec as P


NX, NZ = 4, 16
CAP = 13
TOP = 6
TOK = 128
EXTRA = 8
NEAR = (0, 1, 2, 3, 4, -1, -2, -3)
FAR = (5, 6, 7, -4, -5, -6, -7, 8)
COUNT = len(NEAR)
ROWS = CAP * COUNT
PAD = 128
ZG = [[x * NZ + z for z in range(NZ)] for x in range(NX)]
XG = [[x * NZ + z for x in range(NX)] for z in range(NZ)]


def zperm(d):
    return [(x * NZ + z, x * NZ + (z + d) % NZ) for x in range(NX) for z in range(NZ)]


def pack_body(tokens_ref, ids_ref, gates_ref, out_ref):
    out_ref[:TOK, :] = tokens_ref[...]
    gates = gates_ref[...]
    high = gates.astype(jnp.bfloat16).astype(jnp.float32)
    mid = (gates - high).astype(jnp.bfloat16).astype(jnp.float32)
    low = gates - high - mid
    ids = ids_ref[...].astype(jnp.float32)
    blank = jnp.zeros((EXTRA - 4, TOK), jnp.float32)
    for k in range(TOP):
        at = slice(k, k + 1)
        rows = jnp.concatenate([ids[at], high[at], mid[at], low[at], blank], axis=0)
        out_ref[TOK:, k * TOK : (k + 1) * TOK] = rows.astype(jnp.bfloat16)
    rest = out_ref.shape[1] - TOP * TOK
    out_ref[TOK:, TOP * TOK :] = jnp.zeros((EXTRA, rest), jnp.bfloat16)


def pack(tokens, ids, gates):
    return pl.pallas_call(
        pack_body,
        out_shape=jax.ShapeDtypeStruct((TOK + EXTRA, tokens.shape[1]), jnp.bfloat16),
        cost_estimate=pl.CostEstimate(flops=0, bytes_accessed=4 * TOK * tokens.shape[1], transcendentals=0),
        name="pack",
    )(tokens, ids.T, gates.T)


def pick_rows(code, gate, all_rows, out_ref, weighted):
    slot = lax.broadcasted_iota(jnp.int32, (ROWS, all_rows.shape[0]), 0)
    for j in range(NX):
        hit = slot == code[j : j + 1, :]
        got = jnp.dot(
            jnp.where(hit, 1.0, 0.0).astype(jnp.bfloat16), all_rows, preferred_element_type=jnp.float32
        )
        if weighted:
            got = got * jnp.sum(jnp.where(hit, gate[j : j + 1, :], 0.0), axis=1, keepdims=True)
        out_ref[j] = got.astype(jnp.bfloat16)


def pick_body(place_ref, *refs, spots):
    chunks, (out_ref, code_ref, gate_ref, code_t_ref, gate_t_ref, stage, extra) = refs[:-7], refs[-7:]
    for c, (n, row) in zip(chunks, spots):
        end = row + c.shape[0]
        if end <= TOK:
            stage[n * TOK + row : n * TOK + end, :] = c[...]
        else:
            stage[n * TOK + row : (n + 1) * TOK, :] = c[: TOK - row, :]
            extra[n * EXTRA : (n + 1) * EXTRA, :] = c[TOK - row :, :].astype(jnp.float32)
    mine = place_ref[0] + NZ * lax.broadcasted_iota(jnp.int32, (NX, TOK), 0)
    mine = mine.astype(jnp.float32)
    hits, weights = [], []
    for n in range(COUNT):
        hit = jnp.zeros((NX, TOK), jnp.float32)
        weight = jnp.zeros((NX, TOK), jnp.float32)
        for k in range(TOP):
            part = extra[n * EXTRA : n * EXTRA + 4, k * TOK : (k + 1) * TOK]
            same = part[0:1] == mine
            hit = jnp.where(same, 1.0, hit)
            weight = jnp.where(same, part[1:2] + part[2:3] + part[3:4], weight)
        hits.append(hit)
        weights.append(weight)
    hits, weights = jnp.concatenate(hits, axis=0), jnp.concatenate(weights, axis=0)
    shape = (TOK, TOK)
    earlier = lax.broadcasted_iota(jnp.int32, shape, 0) < lax.broadcasted_iota(jnp.int32, shape, 1)
    position = jnp.dot(
        hits.astype(jnp.bfloat16),
        jnp.where(earlier, 1.0, 0.0).astype(jnp.bfloat16),
        preferred_element_type=jnp.float32,
    )
    first = CAP * (lax.broadcasted_iota(jnp.int32, (NX * COUNT, TOK), 0) // NX)
    codes = jnp.where(hits > 0, position.astype(jnp.int32) + first, -1)
    codes_f = codes.astype(jnp.float32)
    fill = jnp.zeros((TOK - NX * COUNT, TOK), jnp.float32)
    code_t = jnp.concatenate([codes_f, fill], axis=0).T
    gate_t = jnp.concatenate([weights, fill], axis=0).T
    for n in range(COUNT):
        at = slice(n * NX, (n + 1) * NX)
        code_ref[:, n * TOK : (n + 1) * TOK] = codes[at]
        gate_ref[:, n * TOK : (n + 1) * TOK] = weights[at]
        code_t_ref[n] = code_t[:, at]
        gate_t_ref[n] = gate_t[:, at]
    pick_rows(code_ref[...], None, stage[...], out_ref, False)


def pick_cost(rows, width):
    return pl.CostEstimate(
        flops=2 * NX * ROWS * rows * width, bytes_accessed=2 * (rows + NX * ROWS) * width, transcendentals=0
    )


def pick(place, groups):
    pieces, spots = [], []
    for n, group in enumerate(groups):
        row = 0
        for piece in group:
            pieces.append(piece)
            spots.append((n, row))
            row += piece.shape[0]
    width = pieces[0].shape[1]
    rows = COUNT * TOK
    shapes = [((NX, ROWS, width), jnp.bfloat16), ((NX, rows), jnp.int32), ((NX, rows), jnp.float32)]
    shapes += [((COUNT, TOK, NX), jnp.float32)] * 2
    return pl.pallas_call(
        functools.partial(pick_body, spots=spots),
        out_shape=[jax.ShapeDtypeStruct(s, t) for s, t in shapes],
        in_specs=[pl.BlockSpec(memory_space=pltpu.SMEM)] + [pl.BlockSpec(memory_space=pltpu.VMEM)] * len(pieces),
        scratch_shapes=[pltpu.VMEM((rows, width), jnp.bfloat16), pltpu.VMEM((COUNT * EXTRA, width), jnp.float32)],
        cost_estimate=pick_cost(rows, width),
        name="pick",
    )(place, *pieces)


def pick_from_body(source_ref, code_ref, gate_ref, *refs):
    chunks, out_ref, stage = refs[:-2], refs[-2], refs[-1]
    for n, c in enumerate(chunks):
        stage[n * TOK : (n + 1) * TOK, :] = c[...]
    pick_rows(code_ref[...], gate_ref[...], stage[...], out_ref, True)


def pick_from(source, code, gate, gathered):
    width = gathered.shape[1]
    rows = COUNT * TOK
    small = pl.BlockSpec((NX, rows), lambda i, source: (0, 0))
    chunk = [pl.BlockSpec((TOK, width), lambda i, source, n=n: (source[n], 0)) for n in range(COUNT)]
    return pl.pallas_call(
        pick_from_body,
        out_shape=jax.ShapeDtypeStruct((NX, ROWS, width), jnp.bfloat16),
        grid_spec=pltpu.PrefetchScalarGridSpec(
            num_scalar_prefetch=1,
            grid=(1,),
            in_specs=[small, small] + chunk,
            out_specs=pl.BlockSpec((NX, ROWS, width), lambda i, source: (0, 0, 0)),
            scratch_shapes=[pltpu.VMEM((rows, width), jnp.bfloat16)],
        ),
        cost_estimate=pick_cost(rows, width),
        name="pick_weighted",
    )(source, code, gate, *([gathered] * COUNT))


def mix_body(dest_ref, code_ref, gate_ref, rows_ref, *refs):
    out_ref, stage, ready, sems = refs[-4:]
    width = stage.shape[1]
    for j in range(NX):
        stage[j * PAD : j * PAD + ROWS, :] = rows_ref[j]
        stage[j * PAD + ROWS : (j + 1) * PAD, :] = jnp.zeros((PAD - ROWS, width), jnp.bfloat16)
    slot = lax.broadcasted_iota(jnp.int32, (TOK, PAD), 1).astype(jnp.float32)

    def copy(n):
        at = pl.multiple_of(dest_ref[n] * TOK, TOK)
        return pltpu.make_async_copy(ready.at[n], out_ref.at[pl.ds(at, TOK), :], sems.at[n])

    def one(n, carry):
        code, gate = code_ref[n], gate_ref[n]
        full = jnp.concatenate(
            [jnp.where(slot == code[:, j : j + 1], gate[:, j : j + 1], 0.0) for j in range(NX)], axis=1
        )
        high = full.astype(jnp.bfloat16)
        low = (full - high.astype(jnp.float32)).astype(jnp.bfloat16)
        both = jnp.dot(
            jnp.concatenate([high, low], axis=0), stage[...], preferred_element_type=jnp.float32
        )
        ready[n] = (both[:TOK] + both[TOK:]).astype(jnp.bfloat16)
        copy(n).start()
        return carry

    def finish(n, carry):
        copy(n).wait()
        return carry

    lax.fori_loop(0, COUNT, one, 0)
    lax.fori_loop(0, COUNT, finish, 0)


def mix(dest, code_t, gate_t, rows, before):
    width = rows.shape[2]
    chained = before is not None
    vmem = pl.BlockSpec(memory_space=pltpu.VMEM)
    whole = pl.BlockSpec(memory_space=pl.ANY)
    return pl.pallas_call(
        mix_body,
        out_shape=jax.ShapeDtypeStruct((NZ * TOK, width), jnp.bfloat16),
        in_specs=[pl.BlockSpec(memory_space=pltpu.SMEM), vmem, vmem, vmem] + ([whole] if chained else []),
        out_specs=whole,
        scratch_shapes=[
            pltpu.VMEM((NX * PAD, width), jnp.bfloat16),
            pltpu.VMEM((COUNT, TOK, width), jnp.bfloat16),
            pltpu.SemaphoreType.DMA((COUNT,)),
        ],
        input_output_aliases={4: 0} if chained else {},
        cost_estimate=pl.CostEstimate(
            flops=4 * NX * PAD * COUNT * TOK * width,
            bytes_accessed=2 * (NX * ROWS + COUNT * TOK) * width,
            transcendentals=0,
        ),
        name="mix",
    )(dest, code_t, gate_t, rows, *((before,) if chained else ()))


def across_x(blocks):
    return lax.all_to_all(blocks, "ep", split_axis=0, concat_axis=0, axis_index_groups=XG, tiled=True)


def local(tokens, expert_ids, gate_weights, cotangent, w_gate, w_up, w_down):
    width = tokens.shape[1]
    hidden_width = w_gate.shape[2]
    share = w_gate.shape[1]
    z = lax.axis_index("ep") % NZ
    core = lax.axis_index("rep") % 2
    n_rep = lax.axis_size("rep")
    source = (z - jnp.array(NEAR + FAR, jnp.int32)) % NZ
    place = z.reshape(1)
    last = (((1,), (1,)), ((), ()))
    first = (((0,), (0,)), ((), ()))
    tied = lax.optimization_barrier

    fwd = back = pack(tokens, expert_ids, gate_weights)
    held = {0: (fwd,)}

    def step(i):
        nonlocal fwd, back
        sent_fwd, sent_back = fwd, back
        if i > 1:
            sent_fwd, _ = tied((fwd, held[2 - i][0]))
            sent_back, _ = tied((back, held[i - 2][0]))
        fwd = lax.ppermute(sent_fwd, "ep", zperm(1))
        back = lax.ppermute(sent_back, "ep", zperm(-1))
        held[i], held[-i] = (fwd,), (back,)

    def send(b):
        group = (NEAR, FAR)[b]
        rows, code, gate, code_t, gate_t = pick(place, [held[d] for d in group])
        rows = across_x(rows)
        return rows.reshape(NX * ROWS, width), (code, gate), (code_t, gate_t)

    def forward(rows):
        gate_pre = lax.dot_general(rows, full_gate, last, preferred_element_type=jnp.float32)
        up_pre = lax.dot_general(rows, full_up, last, preferred_element_type=jnp.float32)
        silu = jax.nn.silu(gate_pre)
        hidden = (silu * up_pre).astype(jnp.bfloat16)
        out = jnp.dot(hidden, full_down, preferred_element_type=jnp.float32).astype(jnp.bfloat16)
        return out, silu, hidden

    step(1)
    shards = jnp.concatenate([w_gate[0].T, w_up[0].T, w_down[0]], axis=1)
    shards, _, _ = tied((shards, fwd, back))
    shards = jnp.broadcast_to(shards[None], (n_rep,) + shards.shape)
    shards = lax.all_to_all(shards, "rep", split_axis=0, concat_axis=0, tiled=True)
    full_gate, full_up, full_down = (
        shards[:, :, n * share : (n + 1) * share].transpose(1, 0, 2).reshape(hidden_width, width)
        for n in range(3)
    )
    for i in range(2, 6):
        step(i)
    cotangent, _, _ = tied((cotangent, fwd, back))
    all_cot = lax.all_gather(cotangent, "ep", axis_index_groups=ZG, axis=0, tiled=True)
    near_rows, near_routes, near_weights = send(0)
    step(6)
    near_out, near_silu, near_hidden = forward(near_rows)
    near_out, fwd, back = tied((near_out, fwd, back))
    step(7)
    near_back = across_x(near_out.reshape(NX, ROWS, width))
    near_back, fwd, back = tied((near_back, fwd, back))
    mid = TOK // 2
    held[NZ // 2] = (
        lax.ppermute(fwd[:mid], "ep", zperm(1)),
        lax.ppermute(back[mid:], "ep", zperm(-1)),
    )
    far_rows, far_routes, far_weights = send(1)
    mixed = mix(source[:COUNT], *near_weights, near_back, None)
    far_out, far_silu, far_hidden = forward(far_rows)
    mixed = mix(source[COUNT:], *far_weights, across_x(far_out.reshape(NX, ROWS, width)), mixed)
    mixed_out = lax.psum_scatter(mixed, "ep", axis_index_groups=ZG, scatter_dimension=0, tiled=True)

    part_up = part_down = None
    for b, (routes, rows, silu, hidden) in enumerate(
        ((near_routes, near_rows, near_silu, near_hidden), (far_routes, far_rows, far_silu, far_hidden))
    ):
        picked = pick_from(source[b * COUNT : (b + 1) * COUNT], *routes, all_cot)
        grad_rows = across_x(picked).reshape(NX * ROWS, width)
        hidden_grad = lax.dot_general(grad_rows, full_down, last, preferred_element_type=jnp.float32)
        up_grad = (hidden_grad * silu).astype(jnp.bfloat16)
        down = lax.dot_general(grad_rows, hidden, first, preferred_element_type=jnp.float32)
        up = lax.dot_general(rows, up_grad, first, preferred_element_type=jnp.float32)
        part_down = down if part_down is None else part_down + down
        part_up = up if part_up is None else part_up + up

    def summed(part):
        part = part.astype(jnp.bfloat16).reshape(n_rep // 2, 2, width // n_rep, hidden_width)
        kept = lax.dynamic_index_in_dim(part, core, 1, keepdims=False)
        sent = lax.dynamic_index_in_dim(part, 1 - core, 1, keepdims=False)
        swap = [(r, r ^ 1) for r in range(n_rep)]
        got = lax.ppermute(sent, "rep", swap)
        pair = (kept.astype(jnp.float32) + got.astype(jnp.float32)).astype(jnp.bfloat16)
        groups = [list(range(c, n_rep, 2)) for c in range(2)]
        pair = lax.all_to_all(pair, "rep", split_axis=0, concat_axis=0, axis_index_groups=groups, tiled=True)
        return jnp.sum(pair.astype(jnp.float32), axis=0)

    grad_down = summed(part_down).T
    grad_up = summed(part_up)
    return mixed_out, grad_up[None], grad_down[None]


def solution(mesh):
    in_specs = (
        P(("ep", "rep"), None),
        P(("ep", "rep"), None),
        P(("ep", "rep"), None),
        P(("ep", "rep"), None),
        P("ep", "rep", None),
        P("ep", "rep", None),
        P("ep", None, "rep"),
    )
    out_specs = (P(("ep", "rep"), None), P("ep", "rep", None), P("ep", None, "rep"))

    return jax.shard_map(local, mesh=mesh, in_specs=in_specs, out_specs=out_specs, check_vma=False)
```

```python
import functools

import jax
import jax.numpy as jnp
from jax import lax
from jax.experimental import pallas as pl
from jax.experimental.pallas import tpu as pltpu
from jax.sharding import PartitionSpec as P


NX, NZ = 4, 16
CAP = 13
TOP = 6
TOK = 128
EXTRA = 8
NEAR = (0, 1, 2, 3, 4, -1, -2, -3)
FAR = (5, 6, 7, -4, -5, -6, -7, 8)
COUNT = len(NEAR)
ROWS = CAP * COUNT
PAD = 128
STEP = 112
ZG = [[x * NZ + z for z in range(NZ)] for x in range(NX)]
XG = [[x * NZ + z for x in range(NX)] for z in range(NZ)]


def zperm(d):
    return [(x * NZ + z, x * NZ + (z + d) % NZ) for x in range(NX) for z in range(NZ)]


def pack_body(tokens_ref, ids_ref, gates_ref, out_ref):
    out_ref[:TOK, :] = tokens_ref[...]
    gates = gates_ref[...]
    high = gates.astype(jnp.bfloat16).astype(jnp.float32)
    mid = (gates - high).astype(jnp.bfloat16).astype(jnp.float32)
    low = gates - high - mid
    ids = ids_ref[...].astype(jnp.float32)
    blank = jnp.zeros((EXTRA - 4, TOK), jnp.float32)
    for k in range(TOP):
        at = slice(k, k + 1)
        rows = jnp.concatenate([ids[at], high[at], mid[at], low[at], blank], axis=0)
        out_ref[TOK:, k * TOK : (k + 1) * TOK] = rows.astype(jnp.bfloat16)
    rest = out_ref.shape[1] - TOP * TOK
    out_ref[TOK:, TOP * TOK :] = jnp.zeros((EXTRA, rest), jnp.bfloat16)


def pack(tokens, ids, gates):
    return pl.pallas_call(
        pack_body,
        out_shape=jax.ShapeDtypeStruct((TOK + EXTRA, tokens.shape[1]), jnp.bfloat16),
        cost_estimate=pl.CostEstimate(flops=0, bytes_accessed=4 * TOK * tokens.shape[1], transcendentals=0),
        name="pack",
    )(tokens, ids.T, gates.T)


def pick_rows(code, gate, all_rows, out_ref, weighted):
    slot = lax.broadcasted_iota(jnp.int32, (STEP, all_rows.shape[0]), 0)
    hits = [slot == code[j : j + 1, :] for j in range(NX)]
    ones = jnp.concatenate([jnp.where(h, 1.0, 0.0).astype(jnp.bfloat16) for h in hits], axis=0)
    got = jnp.dot(ones, all_rows, preferred_element_type=jnp.float32)
    for j in range(NX):
        part = got[j * STEP : j * STEP + ROWS]
        if weighted:
            scale = jnp.sum(jnp.where(hits[j], gate[j : j + 1, :], 0.0), axis=1, keepdims=True)
            part = part * scale[:ROWS]
        out_ref[j] = part.astype(jnp.bfloat16)


def pick_body(place_ref, *refs, spots):
    chunks, (out_ref, code_ref, gate_ref, code_t_ref, gate_t_ref, stage, extra, found) = refs[:-8], refs[-8:]
    for c, (n, row) in zip(chunks, spots):
        end = row + c.shape[0]
        if end <= TOK:
            stage[n * TOK + row : n * TOK + end, :] = c[...]
        else:
            stage[n * TOK + row : (n + 1) * TOK, :] = c[: TOK - row, :]
            extra[n] = c[TOK - row :, :].astype(jnp.float32)
    mine = place_ref[0] + NZ * lax.broadcasted_iota(jnp.int32, (NX, TOK), 0)
    mine = mine.astype(jnp.float32)

    def match(n, carry):
        rows = extra[n]
        hit = jnp.zeros((NX, TOK), jnp.float32)
        weight = jnp.zeros((NX, TOK), jnp.float32)
        for k in range(TOP):
            part = rows[0:4, k * TOK : (k + 1) * TOK]
            same = part[0:1] == mine
            hit = jnp.where(same, 1.0, hit)
            weight = jnp.where(same, part[1:2] + part[2:3] + part[3:4], weight)
        found[0, n] = hit
        found[1, n] = weight
        return carry

    lax.fori_loop(0, COUNT, match, 0)
    hits = jnp.concatenate([found[0, n] for n in range(COUNT)], axis=0)
    weights = jnp.concatenate([found[1, n] for n in range(COUNT)], axis=0)
    shape = (TOK, TOK)
    earlier = lax.broadcasted_iota(jnp.int32, shape, 0) < lax.broadcasted_iota(jnp.int32, shape, 1)
    position = jnp.dot(
        hits.astype(jnp.bfloat16),
        jnp.where(earlier, 1.0, 0.0).astype(jnp.bfloat16),
        preferred_element_type=jnp.float32,
    )
    first = CAP * (lax.broadcasted_iota(jnp.int32, (NX * COUNT, TOK), 0) // NX)
    codes = jnp.where(hits > 0, position.astype(jnp.int32) + first, -1)
    codes_f = codes.astype(jnp.float32)
    fill = jnp.zeros((TOK - NX * COUNT, TOK), jnp.float32)
    code_t = jnp.concatenate([codes_f, fill], axis=0).T
    gate_t = jnp.concatenate([weights, fill], axis=0).T
    for n in range(COUNT):
        at = slice(n * NX, (n + 1) * NX)
        code_ref[:, n * TOK : (n + 1) * TOK] = codes[at]
        gate_ref[:, n * TOK : (n + 1) * TOK] = weights[at]
        code_t_ref[n] = code_t[:, at]
        gate_t_ref[n] = gate_t[:, at]
    pick_rows(code_ref[...], None, stage[...], out_ref, False)


def pick_cost(rows, width):
    return pl.CostEstimate(
        flops=2 * NX * ROWS * rows * width, bytes_accessed=2 * (rows + NX * ROWS) * width, transcendentals=0
    )


def placed(groups):
    pieces, spots = [], []
    for n, group in enumerate(groups):
        row = 0
        for piece in group:
            pieces.append(piece)
            spots.append((n, row))
            row += piece.shape[0]
    return pieces, spots


def pick(place, groups):
    pieces, spots = placed(groups)
    width = pieces[0].shape[1]
    rows = COUNT * TOK
    shapes = [((NX, ROWS, width), jnp.bfloat16), ((NX, rows), jnp.int32), ((NX, rows), jnp.float32)]
    shapes += [((COUNT, TOK, NX), jnp.float32)] * 2
    return pl.pallas_call(
        functools.partial(pick_body, spots=spots),
        out_shape=[jax.ShapeDtypeStruct(s, t) for s, t in shapes],
        in_specs=[pl.BlockSpec(memory_space=pltpu.SMEM)] + [pl.BlockSpec(memory_space=pltpu.VMEM)] * len(pieces),
        scratch_shapes=[
            pltpu.VMEM((rows, width), jnp.bfloat16),
            pltpu.VMEM((COUNT, EXTRA, width), jnp.float32),
            pltpu.VMEM((2, COUNT, NX, TOK), jnp.float32),
        ],
        cost_estimate=pick_cost(rows, width),
        name="pick",
    )(place, *pieces)


def pick_weighted_body(code_ref, gate_ref, *refs, spots):
    chunks, out_ref, stage = refs[:-2], refs[-2], refs[-1]
    for c, (n, row) in zip(chunks, spots):
        stage[n * TOK + row : n * TOK + row + c.shape[0], :] = c[...]
    pick_rows(code_ref[...], gate_ref[...], stage[...], out_ref, True)


def pick_weighted(code, gate, groups):
    pieces, spots = placed(groups)
    width = pieces[0].shape[1]
    rows = COUNT * TOK
    return pl.pallas_call(
        functools.partial(pick_weighted_body, spots=spots),
        out_shape=jax.ShapeDtypeStruct((NX, ROWS, width), jnp.bfloat16),
        scratch_shapes=[pltpu.VMEM((rows, width), jnp.bfloat16)],
        cost_estimate=pick_cost(rows, width),
        name="pick_weighted",
    )(code, gate, *pieces)


def mix_body(dest_ref, code_ref, gate_ref, rows_ref, *refs):
    out_ref, stage, weights, ready, sems = refs[-5:]
    width = stage.shape[1]
    half = NX * PAD
    blank = jnp.zeros((PAD - ROWS, width), jnp.bfloat16)
    for j in range(NX):
        for at in (j * PAD, half + j * PAD):
            stage[at : at + ROWS, :] = rows_ref[j]
            stage[at + ROWS : at + PAD, :] = blank
    slot = lax.broadcasted_iota(jnp.int32, (TOK, PAD), 1).astype(jnp.float32)

    def weigh(n, carry):
        code, gate = code_ref[n], gate_ref[n]
        at = pl.ds(pl.multiple_of(n * TOK, TOK), TOK)
        for j in range(NX):
            full = jnp.where(slot == code[:, j : j + 1], gate[:, j : j + 1], 0.0)
            high = full.astype(jnp.bfloat16)
            weights[at, j * PAD : (j + 1) * PAD] = high
            weights[at, half + j * PAD : half + (j + 1) * PAD] = (full - high.astype(jnp.float32)).astype(
                jnp.bfloat16
            )
        return carry

    lax.fori_loop(0, COUNT, weigh, 0)

    def copy(n):
        at = pl.multiple_of(dest_ref[n] * TOK, TOK)
        return pltpu.make_async_copy(
            ready.at[pl.ds(n * TOK, TOK), :], out_ref.at[pl.ds(at, TOK), :], sems.at[n]
        )

    some = COUNT // 2
    for part in range(2):
        at = slice(part * some * TOK, (part + 1) * some * TOK)
        ready[at, :] = jnp.dot(weights[at, :], stage[...], preferred_element_type=jnp.float32).astype(jnp.bfloat16)
        for n in range(part * some, (part + 1) * some):
            copy(n).start()
    for n in range(COUNT):
        copy(n).wait()


def mix(dest, code_t, gate_t, rows, before):
    width = rows.shape[2]
    chained = before is not None
    vmem = pl.BlockSpec(memory_space=pltpu.VMEM)
    whole = pl.BlockSpec(memory_space=pl.ANY)
    return pl.pallas_call(
        mix_body,
        out_shape=jax.ShapeDtypeStruct((NZ * TOK, width), jnp.bfloat16),
        in_specs=[pl.BlockSpec(memory_space=pltpu.SMEM), vmem, vmem, vmem] + ([whole] if chained else []),
        out_specs=whole,
        scratch_shapes=[
            pltpu.VMEM((2 * NX * PAD, width), jnp.bfloat16),
            pltpu.VMEM((COUNT * TOK, 2 * NX * PAD), jnp.bfloat16),
            pltpu.VMEM((COUNT * TOK, width), jnp.bfloat16),
            pltpu.SemaphoreType.DMA((COUNT,)),
        ],
        input_output_aliases={4: 0} if chained else {},
        cost_estimate=pl.CostEstimate(
            flops=4 * NX * PAD * COUNT * TOK * width,
            bytes_accessed=2 * (NX * ROWS + COUNT * TOK) * width,
            transcendentals=0,
        ),
        name="mix",
    )(dest, code_t, gate_t, rows, *((before,) if chained else ()))


def across_x(blocks):
    return lax.all_to_all(blocks, "ep", split_axis=0, concat_axis=0, axis_index_groups=XG, tiled=True)


def local(tokens, expert_ids, gate_weights, cotangent, w_gate, w_up, w_down):
    width = tokens.shape[1]
    hidden_width = w_gate.shape[2]
    z = lax.axis_index("ep") % NZ
    n_rep = lax.axis_size("rep")
    source = (z - jnp.array(NEAR + FAR, jnp.int32)) % NZ
    place = z.reshape(1)
    last = (((1,), (1,)), ((), ()))
    first = (((0,), (0,)), ((), ()))
    tied = lax.optimization_barrier

    both = jnp.concatenate([w_gate[0], w_up[0]], axis=1)
    both = lax.all_gather(both, "rep", axis=0, tiled=True)
    full_gate, full_up = both[:, :hidden_width], both[:, hidden_width:]
    full_down = lax.all_gather(w_down[0], "rep", axis=1, tiled=True)

    held = [{0: pack(tokens, expert_ids, gate_weights)}, {0: cotangent}]

    def step(i, after=()):
        for a in range(2):
            mine = held[a]
            for sign in (1, -1):
                sent = mine[sign * (i - 1)]
                waits = list(after)
                if i > 1:
                    waits += [mine[-sign * (i - 2)], *(held[1 - a][s * (i - 2 + a)] for s in (1, -1))]
                sent, *_ = tied((sent, *waits))
                if i < NZ // 2:
                    mine[sign * i] = lax.ppermute(sent, "ep", zperm(sign))
                else:
                    mid = TOK // 2
                    piece = sent[:mid] if sign == 1 else sent[mid:]
                    mine[sign * i] = lax.ppermute(piece, "ep", zperm(sign))

    def chunks(a, group):
        half = NZ // 2
        return [(held[a][half], held[a][-half]) if d == half else (held[a][d],) for d in group]

    def send_tok(group):
        rows, code, gate, code_t, gate_t = pick(place, chunks(0, group))
        rows = across_x(rows)
        return rows.reshape(NX * ROWS, width), (code, gate), (code_t, gate_t)

    def send_cot(group, routes):
        rows = pick_weighted(*routes, chunks(1, group))
        rows = across_x(rows)
        return rows.reshape(NX * ROWS, width)

    def forward(rows):
        gate_pre = jnp.dot(rows, full_gate, preferred_element_type=jnp.float32)
        up_pre = jnp.dot(rows, full_up, preferred_element_type=jnp.float32)
        silu = jax.nn.silu(gate_pre)
        hidden = (silu * up_pre).astype(jnp.bfloat16)
        out = jnp.dot(hidden, full_down, preferred_element_type=jnp.float32).astype(jnp.bfloat16)
        return out.reshape(NX, ROWS, width), silu, hidden

    def backward(rows, grad_rows, silu, hidden):
        hidden_grad = lax.dot_general(grad_rows, full_down, last, preferred_element_type=jnp.float32)
        up_grad = (hidden_grad * silu).astype(jnp.bfloat16)
        down = lax.dot_general(grad_rows, hidden, first, preferred_element_type=jnp.float32)
        up = lax.dot_general(rows, up_grad, first, preferred_element_type=jnp.float32)
        return down, up

    for i in range(1, 6):
        step(i)
    near_rows, near_routes, near_weights = send_tok(NEAR)
    step(6)
    near_grads = send_cot(NEAR, near_routes)
    step(7)
    near_out, near_silu, near_hidden = forward(near_rows)
    step(8, (near_out,))
    near_back = across_x(near_out)
    far_rows, far_routes, far_weights = send_tok(FAR)
    mixed = mix(source[:COUNT], *near_weights, near_back, None)
    far_rows, mixed = tied((far_rows, mixed))
    far_out, far_silu, far_hidden = forward(far_rows)
    far_back = across_x(far_out)
    mixed = mix(source[COUNT:], *far_weights, far_back, mixed)
    mixed_out = lax.psum_scatter(mixed, "ep", axis_index_groups=ZG, scatter_dimension=0, tiled=True)
    far_grads = send_cot(FAR, far_routes)

    near_down, near_up = backward(near_rows, near_grads, near_silu, near_hidden)
    far_down, far_up = backward(far_rows, far_grads, far_silu, far_hidden)

    def summed(part):
        part = part.astype(jnp.bfloat16).reshape(n_rep, width // n_rep, hidden_width)
        part = lax.all_to_all(part, "rep", split_axis=0, concat_axis=0, tiled=True)
        return jnp.sum(part.astype(jnp.float32), axis=0)

    grad_down = summed(near_down + far_down).T
    grad_up = summed(near_up + far_up)
    return mixed_out, grad_up[None], grad_down[None]


def solution(mesh):
    in_specs = (
        P(("ep", "rep"), None),
        P(("ep", "rep"), None),
        P(("ep", "rep"), None),
        P(("ep", "rep"), None),
        P("ep", "rep", None),
        P("ep", "rep", None),
        P("ep", None, "rep"),
    )
    out_specs = (P(("ep", "rep"), None), P("ep", "rep", None), P("ep", None, "rep"))

    return jax.shard_map(local, mesh=mesh, in_specs=in_specs, out_specs=out_specs, check_vma=False)
```

```python
import jax
import jax.numpy as jnp
from jax import lax
from jax.experimental import pallas as pl
from jax.experimental.pallas import tpu as pltpu
from jax.sharding import PartitionSpec as P

NX, NZ = 4, 16
CAP = 13
TOP = 6
TOK = 128
EXTRA = 8
COUNT = NZ // 2
ROWS = CAP * COUNT
PAD = 128
STEP = 112
ZG = [[x * NZ + z for z in range(NZ)] for x in range(NX)]
XG = [[x * NZ + z for x in range(NX)] for z in range(NZ)]


def pack_body(tokens_ref, ids_ref, gates_ref, out_ref):
    out_ref[:TOK, :] = tokens_ref[...]
    gates = gates_ref[...]
    high = gates.astype(jnp.bfloat16).astype(jnp.float32)
    mid = (gates - high).astype(jnp.bfloat16).astype(jnp.float32)
    low = gates - high - mid
    ids = ids_ref[...].astype(jnp.float32)
    blank = jnp.zeros((EXTRA - 4, TOK), jnp.float32)
    for k in range(TOP):
        at = slice(k, k + 1)
        rows = jnp.concatenate([ids[at], high[at], mid[at], low[at], blank], axis=0)
        out_ref[TOK:, k * TOK : (k + 1) * TOK] = rows.astype(jnp.bfloat16)
    rest = out_ref.shape[1] - TOP * TOK
    out_ref[TOK:, TOP * TOK :] = jnp.zeros((EXTRA, rest), jnp.bfloat16)


def pack(tokens, ids, gates):
    return pl.pallas_call(
        pack_body,
        out_shape=jax.ShapeDtypeStruct((TOK + EXTRA, tokens.shape[1]), jnp.bfloat16),
        cost_estimate=pl.CostEstimate(flops=0, bytes_accessed=4 * TOK * tokens.shape[1], transcendentals=0),
        name="pack",
    )(tokens, ids.T, gates.T)


def pick_rows(code, gate, all_rows, out_ref, weighted):
    slot = lax.broadcasted_iota(jnp.int32, (STEP, all_rows.shape[0]), 0)
    hits = [slot == code[j : j + 1, :] for j in range(NX)]
    ones = jnp.concatenate([jnp.where(h, 1.0, 0.0).astype(jnp.bfloat16) for h in hits], axis=0)
    got = jnp.dot(ones, all_rows, preferred_element_type=jnp.float32)
    for j in range(NX):
        part = got[j * STEP : j * STEP + ROWS]
        if weighted:
            scale = jnp.sum(jnp.where(hits[j], gate[j : j + 1, :], 0.0), axis=1, keepdims=True)
            part = part * scale[:ROWS]
        out_ref[j] = part.astype(jnp.bfloat16)


def pick_body(place_ref, all_ref, out_ref, code_ref, gate_ref, code_t_ref, gate_t_ref, stage, extra, found):
    for n in range(COUNT):
        row = n * (TOK + EXTRA)
        stage[n * TOK : (n + 1) * TOK, :] = all_ref[row : row + TOK, :]
        extra[n] = all_ref[row + TOK : row + TOK + EXTRA, :].astype(jnp.float32)
    mine = place_ref[0] + NZ * lax.broadcasted_iota(jnp.int32, (NX, TOK), 0)
    mine = mine.astype(jnp.float32)

    def match(n, carry):
        rows = extra[n]
        hit = jnp.zeros((NX, TOK), jnp.float32)
        weight = jnp.zeros((NX, TOK), jnp.float32)
        for k in range(TOP):
            part = rows[0:4, k * TOK : (k + 1) * TOK]
            same = part[0:1] == mine
            hit = jnp.where(same, 1.0, hit)
            weight = jnp.where(same, part[1:2] + part[2:3] + part[3:4], weight)
        found[0, n] = hit
        found[1, n] = weight
        return carry

    lax.fori_loop(0, COUNT, match, 0)
    hits = jnp.concatenate([found[0, n] for n in range(COUNT)], axis=0)
    weights = jnp.concatenate([found[1, n] for n in range(COUNT)], axis=0)
    shape = (TOK, TOK)
    earlier = lax.broadcasted_iota(jnp.int32, shape, 0) < lax.broadcasted_iota(jnp.int32, shape, 1)
    position = jnp.dot(
        hits.astype(jnp.bfloat16),
        jnp.where(earlier, 1.0, 0.0).astype(jnp.bfloat16),
        preferred_element_type=jnp.float32,
    )
    first = CAP * (lax.broadcasted_iota(jnp.int32, (NX * COUNT, TOK), 0) // NX)
    codes = jnp.where(hits > 0, position.astype(jnp.int32) + first, -1)
    codes_f = codes.astype(jnp.float32)
    fill = jnp.zeros((TOK - NX * COUNT, TOK), jnp.float32)
    code_t = jnp.concatenate([codes_f, fill], axis=0).T
    gate_t = jnp.concatenate([weights, fill], axis=0).T
    for n in range(COUNT):
        at = slice(n * NX, (n + 1) * NX)
        code_ref[:, n * TOK : (n + 1) * TOK] = codes[at]
        gate_ref[:, n * TOK : (n + 1) * TOK] = weights[at]
        code_t_ref[n] = code_t[:, at]
        gate_t_ref[n] = gate_t[:, at]
    pick_rows(code_ref[...], None, stage[...], out_ref, False)


def pick_cost(rows, width):
    return pl.CostEstimate(
        flops=2 * NX * ROWS * rows * width, bytes_accessed=2 * (rows + NX * ROWS) * width, transcendentals=0
    )


def pick(place, gathered, b):
    width = gathered.shape[1]
    rows = COUNT * TOK
    shapes = [((NX, ROWS, width), jnp.bfloat16), ((NX, rows), jnp.int32), ((NX, rows), jnp.float32)]
    shapes += [((COUNT, TOK, NX), jnp.float32)] * 2
    return pl.pallas_call(
        pick_body,
        out_shape=[jax.ShapeDtypeStruct(s, t) for s, t in shapes],
        grid=(1,),
        in_specs=[
            pl.BlockSpec(memory_space=pltpu.SMEM),
            pl.BlockSpec((COUNT * (TOK + EXTRA), width), lambda i: (b, 0)),
        ],
        out_specs=[pl.BlockSpec(s, lambda i, s=s: (0,) * len(s)) for s, _ in shapes],
        scratch_shapes=[
            pltpu.VMEM((rows, width), jnp.bfloat16),
            pltpu.VMEM((COUNT, EXTRA, width), jnp.float32),
            pltpu.VMEM((2, COUNT, NX, TOK), jnp.float32),
        ],
        cost_estimate=pick_cost(rows, width),
        name="pick",
    )(place, gathered)


def pick_weighted_body(code_ref, gate_ref, all_ref, out_ref):
    pick_rows(code_ref[...], gate_ref[...], all_ref[...], out_ref, True)


def pick_weighted(code, gate, gathered, b):
    width = gathered.shape[1]
    rows = COUNT * TOK
    small = pl.BlockSpec((NX, rows), lambda i: (0, 0))
    return pl.pallas_call(
        pick_weighted_body,
        out_shape=jax.ShapeDtypeStruct((NX, ROWS, width), jnp.bfloat16),
        grid=(1,),
        in_specs=[small, small, pl.BlockSpec((rows, width), lambda i: (b, 0))],
        out_specs=pl.BlockSpec((NX, ROWS, width), lambda i: (0, 0, 0)),
        cost_estimate=pick_cost(rows, width),
        name="pick_weighted",
    )(code, gate, gathered)


def mix_body(code_ref, gate_ref, rows_ref, *refs):
    out_ref, stage, weights = refs[-3:]
    width = stage.shape[1]
    half = NX * PAD
    blank = jnp.zeros((PAD - ROWS, width), jnp.bfloat16)
    for j in range(NX):
        for at in (j * PAD, half + j * PAD):
            stage[at : at + ROWS, :] = rows_ref[j]
            stage[at + ROWS : at + PAD, :] = blank
    slot = lax.broadcasted_iota(jnp.int32, (TOK, PAD), 1).astype(jnp.float32)

    def weigh(n, carry):
        code, gate = code_ref[n], gate_ref[n]
        at = pl.ds(pl.multiple_of(n * TOK, TOK), TOK)
        for j in range(NX):
            full = jnp.where(slot == code[:, j : j + 1], gate[:, j : j + 1], 0.0)
            high = full.astype(jnp.bfloat16)
            weights[at, j * PAD : (j + 1) * PAD] = high
            weights[at, half + j * PAD : half + (j + 1) * PAD] = (full - high.astype(jnp.float32)).astype(
                jnp.bfloat16
            )
        return carry

    lax.fori_loop(0, COUNT, weigh, 0)
    out_ref[...] = jnp.dot(weights[...], stage[...], preferred_element_type=jnp.float32).astype(jnp.bfloat16)


def mix(code_t, gate_t, rows, before, b):
    width = rows.shape[2]
    chained = before is not None
    small = pl.BlockSpec((COUNT, TOK, NX), lambda i: (0, 0, 0))
    return pl.pallas_call(
        mix_body,
        out_shape=jax.ShapeDtypeStruct((NZ * TOK, width), jnp.bfloat16),
        grid=(1,),
        in_specs=[small, small, pl.BlockSpec((NX, ROWS, width), lambda i: (0, 0, 0))]
        + ([pl.BlockSpec(memory_space=pl.ANY)] if chained else []),
        out_specs=pl.BlockSpec((COUNT * TOK, width), lambda i: (b, 0)),
        scratch_shapes=[
            pltpu.VMEM((2 * NX * PAD, width), jnp.bfloat16),
            pltpu.VMEM((COUNT * TOK, 2 * NX * PAD), jnp.bfloat16),
        ],
        input_output_aliases={3: 0} if chained else {},
        cost_estimate=pl.CostEstimate(
            flops=4 * NX * PAD * COUNT * TOK * width,
            bytes_accessed=2 * (NX * ROWS + COUNT * TOK) * width,
            transcendentals=0,
        ),
        name="mix",
    )(code_t, gate_t, rows, *((before,) if chained else ()))


def across_x(blocks):
    return lax.all_to_all(blocks, "ep", split_axis=0, concat_axis=0, axis_index_groups=XG, tiled=True)


def local(tokens, expert_ids, gate_weights, cotangent, w_gate, w_up, w_down):
    width = tokens.shape[1]
    hidden_width = w_gate.shape[2]
    share = w_gate.shape[1]
    place = (lax.axis_index("ep") % NZ).reshape(1)
    n_rep = lax.axis_size("rep")
    last = (((1,), (1,)), ((), ()))
    first = (((0,), (0,)), ((), ()))
    tied = lax.optimization_barrier

    def along_z(rows):
        return lax.all_gather(rows, "ep", axis_index_groups=ZG, axis=0, tiled=True)

    with jax.named_scope("tok_gather"):
        all_tok = along_z(pack(tokens, expert_ids, gate_weights))
    with jax.named_scope("cot_gather"):
        all_cot = along_z(cotangent)
    shards = jnp.concatenate([w_gate[0].T, w_up[0].T, w_down[0]], axis=1)
    shards = jnp.broadcast_to(shards[None], (n_rep,) + shards.shape)
    shards = lax.all_to_all(shards, "rep", split_axis=0, concat_axis=0, tiled=True)
    full_gate, full_up, full_down = (
        shards[:, :, n * share : (n + 1) * share].transpose(1, 0, 2).reshape(hidden_width, width)
        for n in range(3)
    )

    def forward(rows):
        gate_pre = lax.dot_general(rows, full_gate, last, preferred_element_type=jnp.float32)
        up_pre = lax.dot_general(rows, full_up, last, preferred_element_type=jnp.float32)
        silu = jax.nn.silu(gate_pre)
        hidden = (silu * up_pre).astype(jnp.bfloat16)
        out = jnp.dot(hidden, full_down, preferred_element_type=jnp.float32).astype(jnp.bfloat16)
        return out.reshape(NX, ROWS, width), silu, hidden

    picked, routes, weights = [], [], []
    for b in range(2):
        rows, code, gate, code_t, gate_t = pick(place, all_tok, b)
        picked.append(across_x(rows).reshape(NX * ROWS, width))
        routes.append((code, gate))
        weights.append((code_t, gate_t))
    outs = [forward(rows) for rows in picked]
    mixed = None
    for b in range(2):
        mixed = mix(*weights[b], across_x(outs[b][0]), mixed, b)
    with jax.named_scope("mixed_scatter"):
        mixed_out = lax.psum_scatter(mixed, "ep", axis_index_groups=ZG, scatter_dimension=0, tiled=True)

    grads = [across_x(pick_weighted(*routes[b], all_cot, b)).reshape(NX * ROWS, width) for b in range(2)]
    part_up = part_down = None
    for b in range(2):
        _, silu, hidden = outs[b]
        down = lax.dot_general(grads[b], hidden, first, preferred_element_type=jnp.float32)
        hidden_grad = lax.dot_general(grads[b], full_down, last, preferred_element_type=jnp.float32)
        up_grad = (hidden_grad * silu).astype(jnp.bfloat16)
        up = lax.dot_general(picked[b], up_grad, first, preferred_element_type=jnp.float32)
        part_down = down if b == 0 else part_down + down
        part_up = up if b == 0 else part_up + up

    def summed(part):
        part = part.astype(jnp.bfloat16).reshape(n_rep, width // n_rep, hidden_width)
        part = lax.all_to_all(part, "rep", split_axis=0, concat_axis=0, tiled=True)
        return jnp.sum(part.astype(jnp.float32), axis=0)

    grad_down = summed(part_down).T
    grad_up = summed(part_up)
    return mixed_out, grad_up[None], grad_down[None]


def solution(mesh):
    in_specs = (
        P(("ep", "rep"), None),
        P(("ep", "rep"), None),
        P(("ep", "rep"), None),
        P(("ep", "rep"), None),
        P("ep", "rep", None),
        P("ep", "rep", None),
        P("ep", None, "rep"),
    )
    out_specs = (P(("ep", "rep"), None), P("ep", "rep", None), P("ep", None, "rep"))
    return jax.shard_map(local, mesh=mesh, in_specs=in_specs, out_specs=out_specs, check_vma=False)
```

```python
import jax
import jax.numpy as jnp
from jax import lax
from jax.experimental import pallas as pl
from jax.experimental.pallas import tpu as pltpu
from jax.sharding import PartitionSpec as P

NX, NZ = 4, 16
CAP = 13
TOP = 6
TOK = 128
EXTRA = 8
COUNT = NZ // 2
ROWS = CAP * COUNT
PAD = 128
STEP = 112
ZG = [[x * NZ + z for z in range(NZ)] for x in range(NX)]
XG = [[x * NZ + z for x in range(NX)] for z in range(NZ)]


def pack_body(tokens_ref, ids_ref, gates_ref, out_ref):
    out_ref[:TOK, :] = tokens_ref[...]
    gates = gates_ref[...]
    high = gates.astype(jnp.bfloat16).astype(jnp.float32)
    mid = (gates - high).astype(jnp.bfloat16).astype(jnp.float32)
    low = gates - high - mid
    ids = ids_ref[...].astype(jnp.float32)
    blank = jnp.zeros((EXTRA - 4, TOK), jnp.float32)
    for k in range(TOP):
        at = slice(k, k + 1)
        rows = jnp.concatenate([ids[at], high[at], mid[at], low[at], blank], axis=0)
        out_ref[TOK:, k * TOK : (k + 1) * TOK] = rows.astype(jnp.bfloat16)
    rest = out_ref.shape[1] - TOP * TOK
    out_ref[TOK:, TOP * TOK :] = jnp.zeros((EXTRA, rest), jnp.bfloat16)


def pack(tokens, ids, gates):
    return pl.pallas_call(
        pack_body,
        out_shape=jax.ShapeDtypeStruct((TOK + EXTRA, tokens.shape[1]), jnp.bfloat16),
        cost_estimate=pl.CostEstimate(flops=0, bytes_accessed=4 * TOK * tokens.shape[1], transcendentals=0),
        name="pack",
    )(tokens, ids.T, gates.T)


def pick_rows(code, gate, all_rows, out_ref, weighted):
    slot = lax.broadcasted_iota(jnp.int32, (STEP, all_rows.shape[0]), 0)
    hits = [slot == code[j : j + 1, :] for j in range(NX)]
    ones = jnp.concatenate([jnp.where(h, 1.0, 0.0).astype(jnp.bfloat16) for h in hits], axis=0)
    got = jnp.dot(ones, all_rows, preferred_element_type=jnp.float32)
    for j in range(NX):
        part = got[j * STEP : j * STEP + ROWS]
        if weighted:
            scale = jnp.sum(jnp.where(hits[j], gate[j : j + 1, :], 0.0), axis=1, keepdims=True)
            part = part * scale[:ROWS]
        out_ref[j] = part.astype(jnp.bfloat16)


def pick_body(place_ref, all_ref, out_ref, code_ref, gate_ref, code_t_ref, gate_t_ref, stage, extra, found):
    for n in range(COUNT):
        row = n * (TOK + EXTRA)
        stage[n * TOK : (n + 1) * TOK, :] = all_ref[row : row + TOK, :]
        extra[n] = all_ref[row + TOK : row + TOK + EXTRA, :].astype(jnp.float32)
    mine = place_ref[0] + NZ * lax.broadcasted_iota(jnp.int32, (NX, TOK), 0)
    mine = mine.astype(jnp.float32)

    def match(n, carry):
        rows = extra[n]
        hit = jnp.zeros((NX, TOK), jnp.float32)
        weight = jnp.zeros((NX, TOK), jnp.float32)
        for k in range(TOP):
            part = rows[0:4, k * TOK : (k + 1) * TOK]
            same = part[0:1] == mine
            hit = jnp.where(same, 1.0, hit)
            weight = jnp.where(same, part[1:2] + part[2:3] + part[3:4], weight)
        found[0, n] = hit
        found[1, n] = weight
        return carry

    lax.fori_loop(0, COUNT, match, 0)
    hits = jnp.concatenate([found[0, n] for n in range(COUNT)], axis=0)
    weights = jnp.concatenate([found[1, n] for n in range(COUNT)], axis=0)
    shape = (TOK, TOK)
    earlier = lax.broadcasted_iota(jnp.int32, shape, 0) < lax.broadcasted_iota(jnp.int32, shape, 1)
    position = jnp.dot(
        hits.astype(jnp.bfloat16),
        jnp.where(earlier, 1.0, 0.0).astype(jnp.bfloat16),
        preferred_element_type=jnp.float32,
    )
    first = CAP * (lax.broadcasted_iota(jnp.int32, (NX * COUNT, TOK), 0) // NX)
    codes = jnp.where(hits > 0, position.astype(jnp.int32) + first, -1)
    codes_f = codes.astype(jnp.float32)
    fill = jnp.zeros((TOK - NX * COUNT, TOK), jnp.float32)
    code_t = jnp.concatenate([codes_f, fill], axis=0).T
    gate_t = jnp.concatenate([weights, fill], axis=0).T
    for n in range(COUNT):
        at = slice(n * NX, (n + 1) * NX)
        code_ref[:, n * TOK : (n + 1) * TOK] = codes[at]
        gate_ref[:, n * TOK : (n + 1) * TOK] = weights[at]
        code_t_ref[n] = code_t[:, at]
        gate_t_ref[n] = gate_t[:, at]
    pick_rows(code_ref[...], None, stage[...], out_ref, False)


def pick_cost(rows, width):
    return pl.CostEstimate(
        flops=2 * NX * ROWS * rows * width, bytes_accessed=2 * (rows + NX * ROWS) * width, transcendentals=0
    )


def pick(place, gathered, b):
    width = gathered.shape[1]
    rows = COUNT * TOK
    shapes = [((NX, ROWS, width), jnp.bfloat16), ((NX, rows), jnp.int32), ((NX, rows), jnp.float32)]
    shapes += [((COUNT, TOK, NX), jnp.float32)] * 2
    return pl.pallas_call(
        pick_body,
        out_shape=[jax.ShapeDtypeStruct(s, t) for s, t in shapes],
        grid=(1,),
        in_specs=[
            pl.BlockSpec(memory_space=pltpu.SMEM),
            pl.BlockSpec((COUNT * (TOK + EXTRA), width), lambda i: (b, 0)),
        ],
        out_specs=[pl.BlockSpec(s, lambda i, s=s: (0,) * len(s)) for s, _ in shapes],
        scratch_shapes=[
            pltpu.VMEM((rows, width), jnp.bfloat16),
            pltpu.VMEM((COUNT, EXTRA, width), jnp.float32),
            pltpu.VMEM((2, COUNT, NX, TOK), jnp.float32),
        ],
        cost_estimate=pick_cost(rows, width),
        name="pick",
    )(place, gathered)


def pick_weighted_body(code_ref, gate_ref, all_ref, out_ref):
    pick_rows(code_ref[...], gate_ref[...], all_ref[...], out_ref, True)


def pick_weighted(code, gate, gathered, b):
    width = gathered.shape[1]
    rows = COUNT * TOK
    small = pl.BlockSpec((NX, rows), lambda i: (0, 0))
    return pl.pallas_call(
        pick_weighted_body,
        out_shape=jax.ShapeDtypeStruct((NX, ROWS, width), jnp.bfloat16),
        grid=(1,),
        in_specs=[small, small, pl.BlockSpec((rows, width), lambda i: (b, 0))],
        out_specs=pl.BlockSpec((NX, ROWS, width), lambda i: (0, 0, 0)),
        cost_estimate=pick_cost(rows, width),
        name="pick_weighted",
    )(code, gate, gathered)


def mix_body(code_ref, gate_ref, rows_ref, *refs):
    out_ref, stage, weights = refs[-3:]
    width = stage.shape[1]
    half = NX * PAD
    blank = jnp.zeros((PAD - ROWS, width), jnp.bfloat16)
    for j in range(NX):
        for at in (j * PAD, half + j * PAD):
            stage[at : at + ROWS, :] = rows_ref[j]
            stage[at + ROWS : at + PAD, :] = blank
    slot = lax.broadcasted_iota(jnp.int32, (TOK, PAD), 1).astype(jnp.float32)

    def weigh(n, carry):
        code, gate = code_ref[n], gate_ref[n]
        at = pl.ds(pl.multiple_of(n * TOK, TOK), TOK)
        for j in range(NX):
            full = jnp.where(slot == code[:, j : j + 1], gate[:, j : j + 1], 0.0)
            high = full.astype(jnp.bfloat16)
            weights[at, j * PAD : (j + 1) * PAD] = high
            weights[at, half + j * PAD : half + (j + 1) * PAD] = (full - high.astype(jnp.float32)).astype(
                jnp.bfloat16
            )
        return carry

    lax.fori_loop(0, COUNT, weigh, 0)
    out_ref[...] = jnp.dot(weights[...], stage[...], preferred_element_type=jnp.float32).astype(jnp.bfloat16)


def mix(code_t, gate_t, rows, before, b):
    width = rows.shape[2]
    chained = before is not None
    small = pl.BlockSpec((COUNT, TOK, NX), lambda i: (0, 0, 0))
    return pl.pallas_call(
        mix_body,
        out_shape=jax.ShapeDtypeStruct((NZ * TOK, width), jnp.bfloat16),
        grid=(1,),
        in_specs=[small, small, pl.BlockSpec((NX, ROWS, width), lambda i: (0, 0, 0))]
        + ([pl.BlockSpec(memory_space=pl.ANY)] if chained else []),
        out_specs=pl.BlockSpec((COUNT * TOK, width), lambda i: (b, 0)),
        scratch_shapes=[
            pltpu.VMEM((2 * NX * PAD, width), jnp.bfloat16),
            pltpu.VMEM((COUNT * TOK, 2 * NX * PAD), jnp.bfloat16),
        ],
        input_output_aliases={3: 0} if chained else {},
        cost_estimate=pl.CostEstimate(
            flops=4 * NX * PAD * COUNT * TOK * width,
            bytes_accessed=2 * (NX * ROWS + COUNT * TOK) * width,
            transcendentals=0,
        ),
        name="mix",
    )(code_t, gate_t, rows, *((before,) if chained else ()))


def split_body(core_ref, part_ref, kept_ref, sent_ref):
    core = core_ref[0]
    count, _, width = kept_ref.shape
    for y in range(count):
        kept_ref[y] = part_ref[:, pl.ds(pl.multiple_of((2 * y + core) * width, width), width)]
        sent_ref[y] = part_ref[:, pl.ds(pl.multiple_of((2 * y + 1 - core) * width, width), width)]


def split(core, part, count):
    height, width = part.shape
    shape = (count, height, width // (2 * count))
    return pl.pallas_call(
        split_body,
        out_shape=[jax.ShapeDtypeStruct(shape, part.dtype)] * 2,
        in_specs=[pl.BlockSpec(memory_space=pltpu.SMEM), pl.BlockSpec(memory_space=pltpu.VMEM)],
        cost_estimate=pl.CostEstimate(flops=0, bytes_accessed=4 * height * width, transcendentals=0),
        name="split",
    )(core, part)


def across_x(blocks):
    return lax.all_to_all(blocks, "ep", split_axis=0, concat_axis=0, axis_index_groups=XG, tiled=True)


def local(tokens, expert_ids, gate_weights, cotangent, w_gate, w_up, w_down):
    width = tokens.shape[1]
    hidden_width = w_gate.shape[2]
    share = w_gate.shape[1]
    place = (lax.axis_index("ep") % NZ).reshape(1)
    n_rep = lax.axis_size("rep")
    last = (((1,), (1,)), ((), ()))
    first = (((0,), (0,)), ((), ()))
    tied = lax.optimization_barrier

    def along_z(rows):
        return lax.all_gather(rows, "ep", axis_index_groups=ZG, axis=0, tiled=True)

    with jax.named_scope("tok_gather"):
        all_tok = along_z(pack(tokens, expert_ids, gate_weights))
    with jax.named_scope("cot_gather"):
        all_cot = along_z(cotangent)
    shards = jnp.concatenate([w_gate[0].T, w_up[0].T, w_down[0]], axis=1)
    shards = jnp.broadcast_to(shards[None], (n_rep,) + shards.shape)
    shards = lax.all_to_all(shards, "rep", split_axis=0, concat_axis=0, tiled=True)
    full_gate, full_up, full_down = (
        shards[:, :, n * share : (n + 1) * share].transpose(1, 0, 2).reshape(hidden_width, width)
        for n in range(3)
    )

    all_tok, full_gate, full_up, full_down = tied((all_tok, full_gate, full_up, full_down))

    def forward(rows):
        gate_pre = lax.dot_general(rows, full_gate, last, preferred_element_type=jnp.float32)
        up_pre = lax.dot_general(rows, full_up, last, preferred_element_type=jnp.float32)
        silu = jax.nn.silu(gate_pre)
        hidden = (silu * up_pre).astype(jnp.bfloat16)
        out = jnp.dot(hidden, full_down, preferred_element_type=jnp.float32).astype(jnp.bfloat16)
        return out.reshape(NX, ROWS, width), silu, hidden

    picked, routes, weights = [], [], []
    for b in range(2):
        rows, code, gate, code_t, gate_t = pick(place, all_tok, b)
        picked.append(across_x(rows).reshape(NX * ROWS, width))
        routes.append((code, gate))
        weights.append((code_t, gate_t))
    outs = [forward(rows) for rows in picked]
    mixed = None
    for b in range(2):
        mixed = mix(*weights[b], across_x(outs[b][0]), mixed, b)
    with jax.named_scope("mixed_scatter"):
        mixed_out = lax.psum_scatter(mixed, "ep", axis_index_groups=ZG, scatter_dimension=0, tiled=True)

    grads = [across_x(pick_weighted(*routes[b], all_cot, b)).reshape(NX * ROWS, width) for b in range(2)]
    def summed(near, far, after=()):
        part = (near + far).astype(jnp.bfloat16)
        kept, sent = split((lax.axis_index("rep") % 2).reshape(1), part, n_rep // 2)
        got = lax.ppermute(sent, "rep", [(r, r ^ 1) for r in range(n_rep)])
        pair = (kept.astype(jnp.float32) + got.astype(jnp.float32)).astype(jnp.bfloat16)
        sent_on, *after = tied((pair, *after))
        groups = [list(range(c, n_rep, 2)) for c in range(2)]
        pair = lax.all_to_all(sent_on, "rep", split_axis=0, concat_axis=0, axis_index_groups=groups, tiled=True)
        return jnp.sum(pair.astype(jnp.float32), axis=0), sent_on, *after

    def down(b):
        return lax.dot_general(outs[b][2], grads[b], first, preferred_element_type=jnp.float32)

    def up(b):
        hidden_grad = lax.dot_general(grads[b], full_down, last, preferred_element_type=jnp.float32)
        up_grad = (hidden_grad * outs[b][1]).astype(jnp.bfloat16)
        return lax.dot_general(up_grad, picked[b], first, preferred_element_type=jnp.float32)

    grad_down, sent_on = summed(down(0), down(1))
    grads[1], _ = tied((grads[1], sent_on))
    grad_up, _, grad_down = summed(up(0), up(1), (grad_down,))
    grad_up = grad_up.T
    return mixed_out, grad_up[None], grad_down[None]


def solution(mesh):
    in_specs = (
        P(("ep", "rep"), None),
        P(("ep", "rep"), None),
        P(("ep", "rep"), None),
        P(("ep", "rep"), None),
        P("ep", "rep", None),
        P("ep", "rep", None),
        P("ep", None, "rep"),
    )
    out_specs = (P(("ep", "rep"), None), P("ep", "rep", None), P("ep", None, "rep"))
    return jax.shard_map(local, mesh=mesh, in_specs=in_specs, out_specs=out_specs, check_vma=False)
```
